128 devices in a mesh: row: 8 (over z, y_lo), col: 16 (over y_hi, x, core).
Axes of the slice: x: 4, y: 4 (y_hi: 2, y_lo: 2; y = y_hi * 2 + y_lo), z: 4, core: 2. Of those that a mesh axis runs over, the one named last changes fastest.
Arguments:
- joined_weight: bfloat16 [16, 2880, 5760], P('row', 'col'), may hold values from -0.109375 to 0.109375
- tile_perm: int32 [144], replicated, may hold values from 0 to 143, each once
- down_weight: bfloat16 [16, 2880, 2880], P('row', 'col'), may hold values from -0.109375 to 0.109375
- tokens: bfloat16 [1024, 2880], P(('row', 'col')), may hold values from -6 to 6
- expert_ids: int32 [1024, 4], replicated, may hold values from 0 to 15, all different within a row; in each aligned block of 1024 rows (0 to 1023, 1024 to 2047, ...) at most 512 rows name the same one
- route_scores: float32 [1024, 4], replicated, may hold values from 0.1 to 1
Outputs:
- gate_weight: bfloat16 [16, 2880, 2880], P('row', None, 'col')
- up_weight: bfloat16 [16, 2880, 2880], P('row', None, 'col')
- mixed: bfloat16 [1024, 2880], P(('row', 'col'))
The draws below stay inside these ranges and needn't reach their ends.
Inputs may be any that keep to these rules, and one draw needn't show every extreme that they name: `expert_ids`: every expert is chosen by at most 512 tokens, a bound that some block reaches.
All inputs are finite; a program needn't handle non-finite values.
Results may differ from the reference program's by a relative error of at most 0.0049.
Values may be sent and summed in bfloat16 or wider, within the bound.
No kernel may reach another device: no remote copies, remote signals or barrier semaphores. Data moves between devices by JAX's collectives and lax.ppermute only.
A program may use at most 128 MiB of HBM per device.

```python
import math
import jax
import jax.numpy as jnp
import numpy as np
from jax import lax

D = 2880
FF = 2880
TOP = 4
EXPERTS = 16
TOKENS = 1024
TILES = 144
CAP = 512


def steps_of(own_key, extent, shards, smallest, top_value):
    factor_of, own = 1.0, jax.random.fold_in(own_key, 6)
    for axis_at, shards_of in shards:
        draws = jnp.exp(jax.random.uniform(jax.random.fold_in(own, axis_at), (shards_of,), jnp.float32, smallest / len(shards), top_value / len(shards)))
        factor_of = factor_of * jnp.repeat(draws, extent[axis_at] // shards_of).reshape([-1 if axis == axis_at else 1 for axis in range(len(extent))])
    return factor_of


def routed_block(key, own, number, rows, amount, top, most, lean):
    sequence = jax.random.permutation(key, amount)
    crowded, ordinary = load_shares(amount, rows * top, most, lean, True), load_shares(amount, rows * top, most, lean, False)
    places = jnp.arange(amount)

    def named(lengths, offset_by):
        used = int((lengths > 0).sum())
        fixed = max(1, used // 4)
        moved = fixed + (places - fixed + offset_by * (used - fixed)) % max(1, amount - fixed)
        return jnp.zeros((amount,), jnp.int32).at[sequence[jnp.where(places < fixed, places, moved)]].set(jnp.asarray(lengths, jnp.int32))

    lengths = jnp.where(number % 4 == 0, named(crowded, number // 4), named(ordinary, number - number // 4 - 1))
    mixed = jax.random.permutation(jax.random.fold_in(own, 3), amount)
    donor, receiver = mixed[0:amount // 2 * 2:2], mixed[1:amount // 2 * 2:2]
    room = jnp.minimum(lengths[donor] - 1, most - lengths[receiver]) // 2
    room = jnp.where((donor == sequence[0]) | (receiver == sequence[0]) | (lengths[receiver] == 0), 0, jnp.maximum(room, 0))
    moved = jax.random.randint(jax.random.fold_in(own, 4), (amount // 2,), 0, 1 << 20) % (room + 1)
    lengths = lengths.at[donor].add(-moved).at[receiver].add(moved)
    members = jnp.searchsorted(jnp.cumsum(lengths), jnp.arange(rows * top), side="right").astype(jnp.int32)
    grid = members.reshape(top, rows).T
    grid = grid[jax.random.permutation(jax.random.fold_in(own, 1), rows)]
    offset_by = jax.random.randint(jax.random.fold_in(own, 2), (rows, 1), 0, top)
    return jnp.take_along_axis(grid, (jnp.arange(top)[None, :] + offset_by) % top, axis=1)


def load_shares(count, total, reach, slope, full):
    loads = [(1 << 20) // math.isqrt(standing ** slope) + 1 for standing in range(1, count + 1)]
    largest = reach if full else min(reach, max(-(-total // count), total * loads[0] // sum(loads)))
    least = 1 if total - largest >= count - 1 else 0
    given, spare = [largest] + [least] * (count - 1), total - largest - least * (count - 1)
    while spare > 0:
        free = [i for i in range(1, count) if given[i] < largest] or [i for i in range(1, count) if given[i] < reach]
        mass, remaining = sum([loads[i] for i in free]), spare
        for i in free:
            more = min(reach - given[i], max(1, remaining * loads[i] // mass), spare)
            given[i] = given[i] + more
            spare = spare - more
    return np.array(given)


def scatter_about(key, extent, deviation, most, shards=(), held_as=jnp.bfloat16):
    loudness = steps_of(key, extent, shards, -0.22, 0.18) if shards else 1.0
    entries = jax.random.normal(key, extent, jnp.float32) * deviation * loudness
    return jnp.minimum(jnp.maximum(entries, -most), most).astype(held_as)


def setup_inputs(seed: int = 0) -> dict:
    arg_keys = jax.random.split(jax.random.key(seed), 7)
    joined_weight = scatter_about(arg_keys[0], (EXPERTS, D, 2 * FF), D ** -0.5, 0.109375, ((0, 8), (1, 16)))
    tile_perm = jax.random.permutation(arg_keys[1], TILES).astype(jnp.int32)
    down_weight = scatter_about(arg_keys[2], (EXPERTS, FF, D), FF ** -0.5, 0.109375, ((0, 8), (1, 16)))
    tokens = scatter_about(arg_keys[3], (TOKENS, D), 1.0, 6.0, ((0, 128),))
    expert_ids_keys = jax.random.split(jax.random.fold_in(arg_keys[4], 1), TOKENS // TOKENS)
    expert_ids_turns = jax.random.permutation(jax.random.fold_in(arg_keys[4], 3), TOKENS // TOKENS)
    expert_ids = jax.vmap(lambda own, number: routed_block(jax.random.fold_in(arg_keys[4], 2), own, number, TOKENS, EXPERTS, TOP, CAP, 0))(expert_ids_keys, expert_ids_turns).reshape((TOKENS, TOP))
    route_scores = jnp.clip(jnp.exp(jax.random.uniform(arg_keys[5], (TOKENS, TOP), jnp.float32, math.log(0.1), math.log(1.0))), 0.1, 1.0)
    return dict(joined_weight=joined_weight, tile_perm=tile_perm, down_weight=down_weight, tokens=tokens, expert_ids=expert_ids, route_scores=route_scores)


def reference(joined_weight, tile_perm, down_weight, tokens, expert_ids, route_scores):
    tiles = tile_perm.shape[0]
    width = joined_weight.shape[2]
    tile_cols = width // tiles
    inverse = jnp.argsort(tile_perm).astype(jnp.int32)
    logical = jnp.arange(width, dtype=jnp.int32)
    stored = inverse[logical // tile_cols] * tile_cols + logical % tile_cols
    ordered = jnp.take(joined_weight, stored, axis=2)
    gate_weight = ordered[:, :, 0::2]
    up_weight = ordered[:, :, 1::2]
    weights = route_scores / jnp.sum(route_scores, axis=1, keepdims=True)

    def add_expert(total, expert):
        share = jnp.sum(weights * (expert_ids == expert), axis=1)
        pre_gate = jnp.dot(tokens, gate_weight[expert], preferred_element_type=jnp.float32)
        pre_up = jnp.dot(tokens, up_weight[expert], preferred_element_type=jnp.float32)
        active = share[:, None] * (pre_up + 1.0) * pre_gate * jax.nn.sigmoid(1.702 * pre_gate)
        active = active.astype(jnp.bfloat16)
        return total + jnp.dot(active, down_weight[expert], preferred_element_type=jnp.float32), None

    start = jnp.zeros((tokens.shape[0], tokens.shape[1]), jnp.float32)
    total, unused = lax.scan(add_expert, start, jnp.arange(joined_weight.shape[0], dtype=jnp.int32))
    return gate_weight, up_weight, total.astype(jnp.bfloat16)
```

```python
import functools

import jax
import jax.numpy as jnp
from jax import lax
from jax.experimental import pallas as pl
from jax.experimental.pallas import tpu as pltpu
from jax.sharding import PartitionSpec as P

BOTH = ("row", "col")


def place_of(i):
    row, col = divmod(i, 16)
    return col // 2 % 4, col // 8 * 2 + row % 2, row // 2, col % 2


def index_of(x, y, z, k):
    x, y, z = x % 4, y % 4, z % 4
    return (z * 2 + y % 2) * 16 + ((y // 2) * 4 + x) * 2 + k


def shifted(a, axis, by):
    pairs = []
    for i in range(128):
        x, y, z, k = place_of(i)
        if axis == "core":
            k = 1 - k
        elif axis == "z":
            z = z + by
        elif (axis == "first") == (k == 0):
            x = x + by
        else:
            y = y + by
        pairs.append((i, index_of(x, y, z, k)))
    return lax.ppermute(a, BOTH, pairs)


def gathered(a, axis):
    return jnp.concatenate([a] + [shifted(a, axis, -by) for by in (1, 2, 3)], axis=0)


def turn_kernel(tile_cols, inverse_ref, x_ref, s_ref, select, turned):
    step = pl.program_id(0)
    span = x_ref.shape[1]
    half = tile_cols // 2
    tiles = s_ref.shape[1] // tile_cols

    @pl.when(step == 0)
    def _():
        out = lax.broadcasted_iota(jnp.int32, (span, span), 0)
        col = lax.broadcasted_iota(jnp.int32, (span, span), 1)
        within = out % tile_cols
        source = out - within + jnp.where(within < half, 2 * within, 2 * (within - half) + 1)
        select[...] = jnp.where(col == source, 1.0, 0.0).astype(select.dtype)

    turned[pl.ds(pl.multiple_of(step * span, 8), span), :] = lax.dot_general(
        select[...], x_ref[...], (((1,), (1,)), ((), ())), preferred_element_type=jnp.float32
    )

    @pl.when(step == pl.num_programs(0) - 1)
    def _():
        def one(j, carry):
            gates, ups = [], []
            for t in range(tiles):
                start = pl.multiple_of(inverse_ref[j * tiles + t] * tile_cols, 8)
                tile = turned[pl.ds(start, tile_cols), :]
                gates.append(tile[:half])
                ups.append(tile[half:])
            s_ref[j] = jnp.concatenate(gates + ups, axis=0).astype(s_ref.dtype)
            return carry

        lax.fori_loop(0, s_ref.shape[0], one, 0)


def join_kernel(depth, r_ref, w_ref):
    for c in range(r_ref.shape[0]):
        w_ref[0, :, c * depth : (c + 1) * depth] = r_ref[c, :, :depth]
        w_ref[1, :, c * depth : (c + 1) * depth] = r_ref[c, :, 192 : 192 + depth]


def body(joined_weight, tile_perm, down_weight, tokens, expert_ids, route_scores):
    n_col = lax.axis_size("col")
    local, depth, width = joined_weight.shape
    tiles = tile_perm.shape[0]
    tile_cols = width // tiles
    mine = width // n_col
    ff = mine // 2
    span = 640
    f32 = jnp.float32

    known = tokens
    for axis in ("second", "first", "z", "core"):
        known = gathered(known, axis) if axis != "core" else jnp.concatenate([known, shifted(known, axis, 1)], axis=0)

    places = jnp.arange(tiles, dtype=jnp.int32)
    inverse = jnp.sum(places[:, None] * (tile_perm[:, None] == places[None, :]), axis=0)
    stacked = jnp.pad(joined_weight, ((0, 0), (0, 192 - depth), (0, 0))).reshape(384, width)
    sent = pl.pallas_call(
        functools.partial(turn_kernel, tile_cols),
        grid_spec=pltpu.PrefetchScalarGridSpec(
            num_scalar_prefetch=1,
            grid=(width // span,),
            in_specs=[pl.BlockSpec((384, span), lambda i, inv: (0, i))],
            out_specs=pl.BlockSpec((n_col, mine, 384), lambda i, inv: (0, 0, 0)),
            scratch_shapes=[pltpu.VMEM((span, span), jnp.bfloat16), pltpu.VMEM((width, 384), f32)],
        ),
        out_shape=jax.ShapeDtypeStruct((n_col, mine, 384), jnp.bfloat16),
        compiler_params=pltpu.CompilerParams(vmem_limit_bytes=48 << 20),
        name="turn",
        cost_estimate=pl.CostEstimate(flops=2 * width * span * 384, bytes_accessed=16 << 20, transcendentals=0),
    )(inverse, stacked)
    came = lax.all_to_all(sent, "col", split_axis=0, concat_axis=0, tiled=True)
    weights_in = pl.pallas_call(
        functools.partial(join_kernel, depth),
        out_shape=jax.ShapeDtypeStruct((local, mine, n_col * depth), jnp.bfloat16),
        compiler_params=pltpu.CompilerParams(vmem_limit_bytes=48 << 20),
        name="join",
        cost_estimate=pl.CostEstimate(flops=1 << 30, bytes_accessed=9 << 20, transcendentals=0),
    )(came)

    me = lax.axis_index(BOTH)
    row, col = me // 16, me % 16
    x, y, z, k = col // 2 % 4, col // 8 * 2 + row % 2, row // 2, col % 2
    at = jnp.arange(1024, dtype=jnp.int32)
    core = (k + at // 512) % 2
    first, second = at // 32 % 4, at // 8 % 4
    own_x = (x + jnp.where(core == 0, first, second)) % 4
    own_y = (y + jnp.where(core == 0, second, first)) % 4
    own_z = (z + at // 128 % 4) % 4
    owner = (own_z * 2 + own_y % 2) * 16 + (own_y // 2 * 4 + own_x) * 2 + core
    token = owner * 8 + at % 8

    expert_global = lax.axis_index("row") * local + jnp.arange(local, dtype=jnp.int32)
    weights = route_scores / jnp.sum(route_scores, axis=1, keepdims=True)
    share = jnp.sum(weights[:, :, None] * (expert_ids[:, :, None] == expert_global[None, None, :]), axis=1)
    share = jnp.take(share, token, axis=0)

    gate_out = jnp.swapaxes(weights_in[:, :ff], 1, 2)
    up_out = jnp.swapaxes(weights_in[:, ff:], 1, 2)
    pre = jnp.einsum("td,nfd->nft", known, weights_in, preferred_element_type=f32)
    pre_gate, pre_up = pre[:, :ff], pre[:, ff:]
    active = share.T[:, None, :] * (pre_up + 1.0) * pre_gate * jax.nn.sigmoid(1.702 * pre_gate)
    active = active.astype(jnp.bfloat16)
    half = active.shape[2] // 2
    other = jnp.einsum("nft,nfd->td", active[:, :, half:], down_weight, preferred_element_type=f32)
    came_over = shifted(other.astype(jnp.bfloat16), "core", 1)
    total = jnp.einsum("nft,nfd->td", active[:, :, :half], down_weight, preferred_element_type=f32)
    total = (total + came_over.astype(f32)).reshape(4, 4, 4, 8, -1)
    parts = [total[:, 0]]
    for by in (1, 2, 3):
        parts.append(shifted(total[:, by].astype(jnp.bfloat16), "first", by).astype(f32))
    total = parts[0] + parts[1] + parts[2] + parts[3]
    parts = [total[:, 0]]
    for by in (1, 2, 3):
        parts.append(shifted(total[:, by].astype(jnp.bfloat16), "second", by).astype(f32))
    total = parts[0] + parts[1] + parts[2] + parts[3]
    parts = [total[0]]
    for by in (1, 2, 3):
        parts.append(shifted(total[by], "z", by))
    total = parts[0] + parts[1] + parts[2] + parts[3]
    return (gate_out, up_out, total.astype(jnp.bfloat16))


def solution(mesh):
    placed = (P("row", "col", None), P(), P("row", "col", None), P(("row", "col"), None), P(), P())
    return jax.shard_map(
        body,
        mesh=mesh,
        in_specs=placed,
        out_specs=(P("row", None, "col"), P("row", None, "col"), P(("row", "col"), None)),
        check_vma=False,
    )
```

```python
import functools

import jax
import jax.numpy as jnp
from jax import lax
from jax.experimental import pallas as pl
from jax.experimental.pallas import tpu as pltpu
from jax.sharding import PartitionSpec as P

BOTH = ("row", "col")


def place_of(i):
    row, col = divmod(i, 16)
    return col // 2 % 4, col // 8 * 2 + row % 2, row // 2, col % 2


def index_of(x, y, z, k):
    x, y, z = x % 4, y % 4, z % 4
    return (z * 2 + y % 2) * 16 + ((y // 2) * 4 + x) * 2 + k


def shifted(a, axis, by):
    pairs = []
    for i in range(128):
        x, y, z, k = place_of(i)
        if axis == "core":
            k = 1 - k
        elif axis == "z":
            z = z + by
        elif (axis == "first") == (k == 0):
            x = x + by
        else:
            y = y + by
        pairs.append((i, index_of(x, y, z, k)))
    return lax.ppermute(a.reshape(-1, 8, a.shape[-1]), BOTH, pairs)


def gathered(a, axis):
    return jnp.concatenate([a.reshape(-1, 8, a.shape[-1])] + [shifted(a, axis, -by) for by in (1, 2, 3)], axis=0)


def turn_kernel(tile_cols, inverse_ref, x_ref, s_ref, turned):
    step = pl.program_id(0)
    local, depth, span = x_ref.shape
    half = tile_cols // 2
    tiles = s_ref.shape[1] // tile_cols
    lanes = 128
    same = lax.broadcasted_iota(jnp.int32, (lanes, lanes), 0) == lax.broadcasted_iota(jnp.int32, (lanes, lanes), 1)
    eye = jnp.where(same, 1.0, 0.0).astype(x_ref.dtype)

    gap = jnp.zeros((192 - depth, lanes), x_ref.dtype)
    for at in range(span // lanes):
        rows = pl.ds(pl.multiple_of(step * span + at * lanes, 8), lanes)
        part = slice(at * lanes, (at + 1) * lanes)
        stacked = jnp.concatenate([piece for e in range(local) for piece in (x_ref[e, :, part], gap)], axis=0)
        flipped = lax.dot_general(eye, stacked, (((1,), (1,)), ((), ())), preferred_element_type=jnp.float32)
        for lane in range(3):
            turned[lane, rows, :] = flipped[:, lane * lanes : (lane + 1) * lanes]

    @pl.when(step == pl.num_programs(0) - 1)
    def _():
        def one(j, carry):
            for lane in range(3):
                pieces = []
                for side in range(2):
                    for t in range(tiles):
                        start = inverse_ref[j * tiles + t] * tile_cols + side
                        pieces.append(turned[lane, pl.ds(start, half, stride=2), :])
                whole = jnp.concatenate(pieces, axis=0).astype(s_ref.dtype)
                s_ref[j, :, lane * lanes : (lane + 1) * lanes] = whole
            return carry

        lax.fori_loop(0, s_ref.shape[0], one, 0)


def join_kernel(depth, r_ref, w_ref):
    for c in range(r_ref.shape[0]):
        w_ref[0, :, c * depth : (c + 1) * depth] = r_ref[c, :, :depth]
        w_ref[1, :, c * depth : (c + 1) * depth] = r_ref[c, :, 192 : 192 + depth]


def experts_kernel(w_ref, t_ref, share_ref, down_ref, out_ref):
    local, ff, width = down_ref.shape
    acts = []
    for e in range(local):
        pre = lax.dot_general(w_ref[e], t_ref[...], (((1,), (1,)), ((), ())), preferred_element_type=jnp.float32)
        gate, up = pre[:ff], pre[ff:]
        act = share_ref[e : e + 1, :] * (up + 1.0) * gate * jax.nn.sigmoid(1.702 * gate)
        acts.append(act.astype(jnp.bfloat16))
    for at in range(0, width, 640):
        part = slice(at, min(at + 640, width))
        out = None
        for e in range(local):
            term = lax.dot_general(
                acts[e], down_ref[e, :, part], (((0,), (0,)), ((), ())), preferred_element_type=jnp.float32
            )
            out = term if out is None else out + term
        for block in range(out_ref.shape[0]):
            to = block % 16 * 4 + block // 16
            out_ref[to, :, part] = out[block * 8 : (block + 1) * 8].astype(out_ref.dtype)


def experts(weights_in, tokens, share, down_weight, dtype):
    rows, width = tokens.shape
    return pl.pallas_call(
        experts_kernel,
        out_shape=jax.ShapeDtypeStruct((rows // 8, 8, width), dtype),
        compiler_params=pltpu.CompilerParams(vmem_limit_bytes=48 << 20),
        name="experts",
        cost_estimate=pl.CostEstimate(flops=3 << 30, bytes_accessed=12 << 20, transcendentals=1 << 18),
    )(weights_in, tokens, share, down_weight)


def body(joined_weight, tile_perm, down_weight, tokens, expert_ids, route_scores):
    n_col = lax.axis_size("col")
    local, depth, width = joined_weight.shape
    tiles = tile_perm.shape[0]
    tile_cols = width // tiles
    mine = width // n_col
    ff = mine // 2
    span = 1152
    f32 = jnp.float32

    places = jnp.arange(tiles, dtype=jnp.int32)
    inverse = jnp.sum(places[:, None] * (tile_perm[:, None] == places[None, :]), axis=0)
    known = gathered(tokens, "second")
    known, joined_weight = lax.optimization_barrier((known, joined_weight))
    known = gathered(known, "first")
    sent = pl.pallas_call(
        functools.partial(turn_kernel, tile_cols),
        grid_spec=pltpu.PrefetchScalarGridSpec(
            num_scalar_prefetch=1,
            grid=(width // span,),
            in_specs=[pl.BlockSpec((local, depth, span), lambda i, inv: (0, 0, i))],
            out_specs=pl.BlockSpec((n_col, mine, 384), lambda i, inv: (0, 0, 0)),
            scratch_shapes=[pltpu.VMEM((3, width, 128), f32)],
        ),
        out_shape=jax.ShapeDtypeStruct((n_col, mine, 384), jnp.bfloat16),
        compiler_params=pltpu.CompilerParams(vmem_limit_bytes=48 << 20),
        name="turn",
        cost_estimate=pl.CostEstimate(flops=4 << 30, bytes_accessed=16 << 20, transcendentals=0),
    )(inverse, joined_weight)
    known, sent = lax.optimization_barrier((known, sent))
    came = lax.all_to_all(sent, "col", split_axis=0, concat_axis=0, tiled=True)
    known = gathered(known, "z")
    known_other = shifted(known, "core", 1)
    weights_in = pl.pallas_call(
        functools.partial(join_kernel, depth),
        out_shape=jax.ShapeDtypeStruct((local, mine, n_col * depth), jnp.bfloat16),
        compiler_params=pltpu.CompilerParams(vmem_limit_bytes=48 << 20),
        name="join",
        cost_estimate=pl.CostEstimate(flops=1 << 30, bytes_accessed=9 << 20, transcendentals=0),
    )(came)

    me = lax.axis_index(BOTH)
    row, col = me // 16, me % 16
    x, y, z, k = col // 2 % 4, col // 8 * 2 + row % 2, row // 2, col % 2
    at = jnp.arange(1024, dtype=jnp.int32)
    core = (k + at // 512) % 2
    first, second = at // 32 % 4, at // 8 % 4
    own_x = (x + jnp.where(core == 0, first, second)) % 4
    own_y = (y + jnp.where(core == 0, second, first)) % 4
    own_z = (z + at // 128 % 4) % 4
    owner = (own_z * 2 + own_y % 2) * 16 + (own_y // 2 * 4 + own_x) * 2 + core
    token = owner * 8 + at % 8

    expert_global = lax.axis_index("row") * local + jnp.arange(local, dtype=jnp.int32)
    weights = route_scores / jnp.sum(route_scores, axis=1, keepdims=True)
    share = jnp.sum(weights[:, :, None] * (expert_ids[:, :, None] == expert_global[None, None, :]), axis=1)
    share = jnp.take(share, token, axis=0)

    gate_out = jnp.swapaxes(weights_in[:, :ff], 1, 2)
    up_out = jnp.swapaxes(weights_in[:, ff:], 1, 2)
    share = share.T
    known, known_other = (a.reshape(-1, a.shape[-1]) for a in (known, known_other))
    other = experts(weights_in, known_other, share[:, 512:], down_weight, jnp.bfloat16)
    came_over = shifted(other, "core", 1)
    total = experts(weights_in, known, share[:, :512], down_weight, f32)
    total = total + came_over.astype(f32)
    for axis, sent_as in (("first", jnp.bfloat16), ("second", jnp.bfloat16), ("z", f32)):
        total = total.reshape(4, -1, 8, total.shape[-1])
        parts = [shifted(total[by].astype(sent_as), axis, by).astype(f32) for by in (1, 2, 3)]
        total = total[0] + parts[0] + parts[1] + parts[2]
    total = total.reshape(8, -1)
    return (gate_out, up_out, total.astype(jnp.bfloat16))


def solution(mesh):
    placed = (P("row", "col", None), P(), P("row", "col", None), P(("row", "col"), None), P(), P())
    return jax.shard_map(
        body,
        mesh=mesh,
        in_specs=placed,
        out_specs=(P("row", None, "col"), P("row", None, "col"), P(("row", "col"), None)),
        check_vma=False,
    )
```

```python
import functools

import jax
import jax.numpy as jnp
from jax import lax
from jax.experimental import pallas as pl
from jax.experimental.pallas import tpu as pltpu
from jax.sharding import PartitionSpec as P

BOTH = ("row", "col")


def place_of(i):
    row, col = divmod(i, 16)
    return col // 2 % 4, col // 8 * 2 + row % 2, row // 2, col % 2


def index_of(x, y, z, k):
    x, y, z = x % 4, y % 4, z % 4
    return (z * 2 + y % 2) * 16 + ((y // 2) * 4 + x) * 2 + k


def shifted(a, axis, by):
    pairs = []
    for i in range(128):
        x, y, z, k = place_of(i)
        if axis == "core":
            k = 1 - k
        elif axis == "z":
            z = z + by
        elif (axis == "first") == (k == 0):
            x = x + by
        else:
            y = y + by
        pairs.append((i, index_of(x, y, z, k)))
    return lax.ppermute(a.reshape(-1, 8, a.shape[-1]), BOTH, pairs)


def gathered(a, axis):
    return jnp.concatenate([a.reshape(-1, 8, a.shape[-1])] + [shifted(a, axis, -by) for by in (1, 2, 3)], axis=0)


def turn_kernel(tile_cols, inverse_ref, x_ref, s_ref, turned):
    step = pl.program_id(0)
    local, depth, span = x_ref.shape
    half = tile_cols // 2
    tiles = s_ref.shape[1] // tile_cols
    lanes = 128
    same = lax.broadcasted_iota(jnp.int32, (lanes, lanes), 0) == lax.broadcasted_iota(jnp.int32, (lanes, lanes), 1)
    eye = jnp.where(same, 1.0, 0.0).astype(x_ref.dtype)

    gap = jnp.zeros((192 - depth, lanes), x_ref.dtype)
    for at in range(span // lanes):
        rows = pl.ds(pl.multiple_of(step * span + at * lanes, 8), lanes)
        part = slice(at * lanes, (at + 1) * lanes)
        stacked = jnp.concatenate([piece for e in range(local) for piece in (x_ref[e, :, part], gap)], axis=0)
        flipped = lax.dot_general(eye, stacked, (((1,), (1,)), ((), ())), preferred_element_type=jnp.float32)
        for lane in range(3):
            turned[lane, rows, :] = flipped[:, lane * lanes : (lane + 1) * lanes]

    @pl.when(step == pl.num_programs(0) - 1)
    def _():
        def one(j, carry):
            for lane in range(3):
                pieces = []
                for side in range(2):
                    for t in range(tiles):
                        start = inverse_ref[j * tiles + t] * tile_cols + side
                        pieces.append(turned[lane, pl.ds(start, half, stride=2), :])
                whole = jnp.concatenate(pieces, axis=0).astype(s_ref.dtype)
                s_ref[j, :, lane * lanes : (lane + 1) * lanes] = whole
            return carry

        lax.fori_loop(0, s_ref.shape[0], one, 0)


def activated(w, t, share):
    ff = w.shape[0] // 2
    pre = lax.dot_general(w, t, (((1,), (1,)), ((), ())), preferred_element_type=jnp.float32)
    gate, up = pre[:ff], pre[ff:]
    act = share * (up + 1.0) * gate * jax.nn.sigmoid(1.702 * gate)
    return act.astype(jnp.bfloat16).T


def hidden_kernel(w_ref, t_ref, share_ref, act_ref):
    for e in range(act_ref.shape[0]):
        act_ref[e] = activated(w_ref[e], t_ref[...], share_ref[e : e + 1, :])


def hidden(weights_in, tokens, share):
    local, mine, width = weights_in.shape
    rows, part = tokens.shape[0], 256
    return pl.pallas_call(
        hidden_kernel,
        grid=(rows // part,),
        in_specs=[
            pl.BlockSpec(weights_in.shape, lambda i: (0, 0, 0)),
            pl.BlockSpec((part, width), lambda i: (i, 0)),
            pl.BlockSpec((local, part), lambda i: (0, i)),
        ],
        out_specs=pl.BlockSpec((local, part, mine // 2), lambda i: (0, i, 0)),
        out_shape=jax.ShapeDtypeStruct((local, rows, mine // 2), jnp.bfloat16),
        compiler_params=pltpu.CompilerParams(vmem_limit_bytes=20 << 20),
        name="hidden",
        cost_estimate=pl.CostEstimate(flops=2 << 30, bytes_accessed=8 << 20, transcendentals=1 << 18),
    )(weights_in, tokens, share)


def projected(acts, downs):
    out = None
    for act, down in zip(acts, downs):
        term = jnp.dot(act, down, preferred_element_type=jnp.float32)
        out = term if out is None else out + term
    return out


def moved(block):
    return block % 16 * 4 + block // 16


def other_kernel(r_ref, t_ref, share_ref, down_ref, w_ref, out_ref, r_in, t_in, sems):
    sources, mine, _ = r_ref.shape
    local, ff, width = down_ref.shape
    depth = width // sources
    tokens_in = pltpu.make_async_copy(t_ref, t_in, sems.at[sources])
    pieces = [pltpu.make_async_copy(r_ref.at[c], r_in.at[c], sems.at[c]) for c in range(sources)]
    for piece in pieces:
        piece.start()
    tokens_in.start()
    for c, piece in enumerate(pieces):
        piece.wait()
        for e in range(local):
            w_ref[e, :, c * depth : (c + 1) * depth] = r_in[c, :, e * 192 : e * 192 + depth]
    tokens_in.wait()
    acts = [activated(w_ref[e], t_in[...], share_ref[e : e + 1, :]) for e in range(local)]
    for at in range(0, width, 640):
        part = slice(at, min(at + 640, width))
        out = projected(acts, [down_ref[e, :, part] for e in range(local)])
        for block in range(out_ref.shape[0]):
            out_ref[moved(block), :, part] = out[block * 8 : (block + 1) * 8].astype(out_ref.dtype)


def emit_kernel(w_ref, gate_ref, up_ref):
    ff = gate_ref.shape[0]
    for e in range(w_ref.shape[0]):
        gate_ref[:, e, :] = w_ref[e, :ff, :]
        up_ref[:, e, :] = w_ref[e, ff:, :]


def own_kernel(act_ref, down_ref, came_ref, *out_refs):
    local, _, width = down_ref.shape
    acts = [act_ref[e] for e in range(local)]
    for at in range(0, width, 640):
        part = slice(at, min(at + 640, width))
        out = projected(acts, [down_ref[e, :, part] for e in range(local)])
        for block in range(came_ref.shape[0]):
            to = moved(block)
            both = out[block * 8 : (block + 1) * 8] + came_ref[to, :, part].astype(jnp.float32)
            ref = out_refs[to // 16]
            ref[to % 16, :, part] = both.astype(ref.dtype)


def own_call(act, down_weight, came, outs):
    vmem = pl.BlockSpec(memory_space=pltpu.VMEM)
    return pl.pallas_call(
        own_kernel,
        in_specs=[vmem] * 3,
        out_specs=[vmem] * len(outs),
        out_shape=outs,
        compiler_params=pltpu.CompilerParams(vmem_limit_bytes=20 << 20),
        name="down_own",
        cost_estimate=pl.CostEstimate(flops=1 << 30, bytes_accessed=8 << 20, transcendentals=0),
    )(act, down_weight, came)


def body(joined_weight, tile_perm, down_weight, tokens, expert_ids, route_scores):
    n_col = lax.axis_size("col")
    local, depth, width = joined_weight.shape
    tiles = tile_perm.shape[0]
    tile_cols = width // tiles
    mine = width // n_col
    ff = mine // 2
    span = 1152
    f32 = jnp.float32

    places = jnp.arange(tiles, dtype=jnp.int32)
    inverse = jnp.sum(places[:, None] * (tile_perm[:, None] == places[None, :]), axis=0)
    known = gathered(tokens, "second")
    known, inverse = lax.optimization_barrier((known, inverse))
    known = gathered(known, "first")
    sent = pl.pallas_call(
        functools.partial(turn_kernel, tile_cols),
        grid_spec=pltpu.PrefetchScalarGridSpec(
            num_scalar_prefetch=1,
            grid=(width // span,),
            in_specs=[pl.BlockSpec((local, depth, span), lambda i, inv: (0, 0, i))],
            out_specs=pl.BlockSpec((n_col, mine, 384), lambda i, inv: (0, 0, 0)),
            scratch_shapes=[pltpu.VMEM((3, width, 128), f32)],
        ),
        out_shape=jax.ShapeDtypeStruct((n_col, mine, 384), jnp.bfloat16),
        compiler_params=pltpu.CompilerParams(vmem_limit_bytes=48 << 20),
        name="turn",
        cost_estimate=pl.CostEstimate(flops=4 << 30, bytes_accessed=16 << 20, transcendentals=0),
    )(inverse, joined_weight)
    known, sent = lax.optimization_barrier((known, sent))
    came = lax.all_to_all(sent, "col", split_axis=0, concat_axis=0, tiled=True)
    known = gathered(known, "z")
    known_other = shifted(known, "core", 1)
    me = lax.axis_index(BOTH)
    row, col = me // 16, me % 16
    x, y, z, k = col // 2 % 4, col // 8 * 2 + row % 2, row // 2, col % 2
    at = jnp.arange(1024, dtype=jnp.int32)
    core = (k + at // 512) % 2
    first, second = at // 32 % 4, at // 8 % 4
    own_x = (x + jnp.where(core == 0, first, second)) % 4
    own_y = (y + jnp.where(core == 0, second, first)) % 4
    own_z = (z + at // 128 % 4) % 4
    owner = (own_z * 2 + own_y % 2) * 16 + (own_y // 2 * 4 + own_x) * 2 + core
    token = owner * 8 + at % 8

    expert_global = lax.axis_index("row") * local + jnp.arange(local, dtype=jnp.int32)
    weights = route_scores / jnp.sum(route_scores, axis=1, keepdims=True)
    share = jnp.sum(weights[:, :, None] * (expert_ids[:, :, None] == expert_global[None, None, :]), axis=1)
    share = jnp.take(share, token, axis=0)

    share = share.T
    known, known_other = (a.reshape(-1, a.shape[-1]) for a in (known, known_other))
    width = known.shape[1]

    def blocks(n, dtype):
        return jax.ShapeDtypeStruct((n, 8, width), dtype)

    vmem = pl.BlockSpec(memory_space=pltpu.VMEM)
    weights_in, other = pl.pallas_call(
        other_kernel,
        in_specs=[pl.BlockSpec(memory_space=pl.ANY), pl.BlockSpec(memory_space=pl.ANY), vmem, vmem],
        out_specs=[vmem, vmem],
        out_shape=[jax.ShapeDtypeStruct((local, mine, width), jnp.bfloat16), blocks(64, jnp.bfloat16)],
        scratch_shapes=[
            pltpu.VMEM(came.shape, jnp.bfloat16),
            pltpu.VMEM(known_other.shape, jnp.bfloat16),
            pltpu.SemaphoreType.DMA((n_col + 1,)),
        ],
        compiler_params=pltpu.CompilerParams(vmem_limit_bytes=32 << 20),
        name="other",
        cost_estimate=pl.CostEstimate(flops=4 << 30, bytes_accessed=16 << 20, transcendentals=1 << 18),
    )(came, known_other, share[:, 512:], down_weight)
    came_over = shifted(other, "core", 1)
    act = hidden(weights_in, known, share[:, :512])
    outs = [blocks(16, f32)] + [blocks(16, jnp.bfloat16)] * 3
    total, *parts = own_call(act, down_weight, came_over, outs)
    weights_in, total = lax.optimization_barrier((weights_in, total))
    unit_major = jax.ShapeDtypeStruct((ff, local, width), jnp.bfloat16)
    gate_out, up_out = (
        a.transpose(1, 2, 0)
        for a in pl.pallas_call(
            emit_kernel,
            out_shape=[unit_major, unit_major],
            compiler_params=pltpu.CompilerParams(vmem_limit_bytes=20 << 20),
            name="emit",
            cost_estimate=pl.CostEstimate(flops=2 << 30, bytes_accessed=8 << 20, transcendentals=0),
        )(weights_in)
    )
    parts = [shifted(parts[by - 1], "first", by).astype(f32) for by in (1, 2, 3)]
    total = total + parts[0] + parts[1] + parts[2]
    total, gate_out, up_out = lax.optimization_barrier((total, gate_out, up_out))
    for axis, sent_as in (("second", jnp.bfloat16), ("z", f32)):
        total = total.reshape(4, -1, 8, width)
        parts = [shifted(total[by].astype(sent_as), axis, by).astype(f32) for by in (1, 2, 3)]
        total = total[0] + parts[0] + parts[1] + parts[2]
    total = total.reshape(8, width)
    return (gate_out, up_out, total.astype(jnp.bfloat16))


def solution(mesh):
    placed = (P("row", "col", None), P(), P("row", "col", None), P(("row", "col"), None), P(), P())
    return jax.shard_map(
        body,
        mesh=mesh,
        in_specs=placed,
        out_specs=(P("row", None, "col"), P("row", None, "col"), P(("row", "col"), None)),
        check_vma=False,
    )
```

```python
import functools

import jax
import jax.numpy as jnp
from jax import lax
from jax.experimental import pallas as pl
from jax.experimental.pallas import tpu as pltpu
from jax.sharding import PartitionSpec as P


BOTH = ("row", "col")


def place_of(i):
    row, col = divmod(i, 16)
    return col // 2 % 4, col // 8 * 2 + row % 2, row // 2, col % 2


def index_of(x, y, z, k):
    x, y, z = x % 4, y % 4, z % 4
    return (z * 2 + y % 2) * 16 + ((y // 2) * 4 + x) * 2 + k


def shifted(a, axis, by):
    pairs = []
    for i in range(128):
        x, y, z, k = place_of(i)
        if axis == "core":
            k = 1 - k
        elif axis == "z":
            z = z + by
        elif (axis == "first") == (k == 0):
            x = x + by
        else:
            y = y + by
        pairs.append((i, index_of(x, y, z, k)))
    return lax.ppermute(a.reshape(-1, 8, a.shape[-1]), BOTH, pairs)


def gathered(a, axis):
    return jnp.concatenate([a.reshape(-1, 8, a.shape[-1])] + [shifted(a, axis, -by) for by in (1, 2, 3)], axis=0)


def turn_kernel(tile_cols, inverse_ref, me_ref, x_ref, *refs):
    s_refs, (turned, staged, sems) = refs[:-3], refs[-3:]
    step = pl.program_id(0)
    local, depth, span = x_ref.shape
    half = tile_cols // 2
    tiles = s_refs[0].shape[0] // tile_cols
    lanes = 128
    same = lax.broadcasted_iota(jnp.int32, (lanes, lanes), 0) == lax.broadcasted_iota(jnp.int32, (lanes, lanes), 1)
    eye = jnp.where(same, 1.0, 0.0).astype(x_ref.dtype)

    gap = jnp.zeros((192 - depth, lanes), x_ref.dtype)
    for at in range(span // lanes):
        rows = pl.ds(pl.multiple_of(step * span + at * lanes, 8), lanes)
        part = slice(at * lanes, (at + 1) * lanes)
        stacked = jnp.concatenate([piece for e in range(local) for piece in (x_ref[e, :, part], gap)], axis=0)
        flipped = lax.dot_general(eye, stacked, (((1,), (1,)), ((), ())), preferred_element_type=jnp.float32)
        for lane in range(3):
            turned[lane, rows, :] = flipped[:, lane * lanes : (lane + 1) * lanes]

    @pl.when(step == pl.num_programs(0) - 1)
    def _():
        copies = []
        for n, s_ref in enumerate(s_refs):
            first = (me_ref[0] ^ n) * tiles
            starts = [inverse_ref[first + t] * tile_cols for t in range(tiles)]
            for lane in range(3):
                pieces = [
                    turned[lane, pl.ds(start + side, half, stride=2), :] for side in range(2) for start in starts
                ]
                whole = jnp.concatenate(pieces, axis=0).astype(staged.dtype)
                staged[n, :, lane * lanes : (lane + 1) * lanes] = whole
            copies.append(pltpu.make_async_copy(staged.at[n], s_ref, sems.at[n]))
            copies[-1].start()
        for copy in copies:
            copy.wait()


def activated(w, t, share):
    ff = w.shape[0] // 2
    pre = lax.dot_general(w, t, (((1,), (1,)), ((), ())), preferred_element_type=jnp.float32)
    gate, up = pre[:ff], pre[ff:]
    act = share * (up + 1.0) * gate * jax.nn.sigmoid(1.702 * gate)
    return act.astype(jnp.bfloat16).T


def hidden_kernel(w_ref, t_ref, share_ref, act_ref):
    for e in range(act_ref.shape[0]):
        act_ref[e] = activated(w_ref[e], t_ref[...], share_ref[e : e + 1, :])


def hidden(weights_in, tokens, share):
    local, mine, width = weights_in.shape
    rows, part = tokens.shape[0], 256
    return pl.pallas_call(
        hidden_kernel,
        grid=(rows // part,),
        in_specs=[
            pl.BlockSpec(weights_in.shape, lambda i: (0, 0, 0)),
            pl.BlockSpec((part, width), lambda i: (i, 0)),
            pl.BlockSpec((local, part), lambda i: (0, i)),
        ],
        out_specs=pl.BlockSpec((local, part, mine // 2), lambda i: (0, i, 0)),
        out_shape=jax.ShapeDtypeStruct((local, rows, mine // 2), jnp.bfloat16),
        compiler_params=pltpu.CompilerParams(vmem_limit_bytes=20 << 20),
        name="hidden",
        cost_estimate=pl.CostEstimate(flops=2 << 30, bytes_accessed=8 << 20, transcendentals=1 << 18),
    )(weights_in, tokens, share)


def projected(acts, downs):
    out = None
    for act, down in zip(acts, downs):
        term = jnp.dot(act, down, preferred_element_type=jnp.float32)
        out = term if out is None else out + term
    return out


def moved(block):
    return block % 16 * 4 + block // 16


def other_kernel(sources, me_ref, *refs):
    r_refs, (t_ref, share_ref, down_ref, w_ref, out_ref, r_in, t_in, sems) = refs[:sources], refs[sources:]
    local, _, width = down_ref.shape
    depth = width // sources
    for n, r_ref in enumerate(r_refs):
        slot = me_ref[0] ^ n
        pltpu.make_async_copy(r_ref, r_in.at[slot], sems.at[slot]).start()
    tokens_in = pltpu.make_async_copy(t_ref, t_in, sems.at[sources])
    tokens_in.start()
    for c in range(sources):
        pltpu.make_async_copy(r_refs[0], r_in.at[c], sems.at[c]).wait()
        for e in range(local):
            w_ref[e, :, c * depth : (c + 1) * depth] = r_in[c, :, e * 192 : e * 192 + depth]
    tokens_in.wait()
    acts = [activated(w_ref[e], t_in[...], share_ref[e : e + 1, :]) for e in range(local)]
    for at in range(0, width, 640):
        part = slice(at, min(at + 640, width))
        out = projected(acts, [down_ref[e, :, part] for e in range(local)])
        for block in range(out_ref.shape[0]):
            out_ref[moved(block), :, part] = out[block * 8 : (block + 1) * 8].astype(out_ref.dtype)


def emit_kernel(w_ref, gate_ref, up_ref):
    ff = gate_ref.shape[0]
    for e in range(w_ref.shape[0]):
        gate_ref[:, e, :] = w_ref[e, :ff, :]
        up_ref[:, e, :] = w_ref[e, ff:, :]


def own_kernel(act_ref, down_ref, came_ref, *out_refs):
    local, _, width = down_ref.shape
    acts = [act_ref[e] for e in range(local)]
    for at in range(0, width, 640):
        part = slice(at, min(at + 640, width))
        out = projected(acts, [down_ref[e, :, part] for e in range(local)])
        for block in range(came_ref.shape[0]):
            to = moved(block)
            both = out[block * 8 : (block + 1) * 8] + came_ref[to, :, part].astype(jnp.float32)
            ref = out_refs[to // 16]
            ref[to % 16, :, part] = both.astype(ref.dtype)


def own_call(act, down_weight, came, outs):
    vmem = pl.BlockSpec(memory_space=pltpu.VMEM)
    return pl.pallas_call(
        own_kernel,
        in_specs=[vmem] * 3,
        out_specs=[vmem] * len(outs),
        out_shape=outs,
        compiler_params=pltpu.CompilerParams(vmem_limit_bytes=20 << 20),
        name="down_own",
        cost_estimate=pl.CostEstimate(flops=1 << 30, bytes_accessed=8 << 20, transcendentals=0),
    )(act, down_weight, came)


def body(joined_weight, tile_perm, down_weight, tokens, expert_ids, route_scores):
    n_col = lax.axis_size("col")
    local, depth, width = joined_weight.shape
    tiles = tile_perm.shape[0]
    tile_cols = width // tiles
    mine = width // n_col
    ff = mine // 2
    span = 1152
    f32 = jnp.float32

    places = jnp.arange(tiles, dtype=jnp.int32)
    inverse = jnp.sum(places[:, None] * (tile_perm[:, None] == places[None, :]), axis=0)
    known = gathered(tokens, "second")
    known, inverse = lax.optimization_barrier((known, inverse))
    known = gathered(known, "first")
    me_col = lax.axis_index("col")[None]
    sent = pl.pallas_call(
        functools.partial(turn_kernel, tile_cols),
        grid_spec=pltpu.PrefetchScalarGridSpec(
            num_scalar_prefetch=2,
            grid=(width // span,),
            in_specs=[pl.BlockSpec((local, depth, span), lambda i, inv, me: (0, 0, i))],
            out_specs=[pl.BlockSpec(memory_space=pltpu.HBM)] * n_col,
            scratch_shapes=[
                pltpu.VMEM((3, width, 128), f32),
                pltpu.VMEM((n_col, mine, 384), jnp.bfloat16),
                pltpu.SemaphoreType.DMA((n_col,)),
            ],
        ),
        out_shape=[jax.ShapeDtypeStruct((mine, 384), jnp.bfloat16)] * n_col,
        compiler_params=pltpu.CompilerParams(vmem_limit_bytes=24 << 20),
        name="turn",
        cost_estimate=pl.CostEstimate(flops=4 << 30, bytes_accessed=16 << 20, transcendentals=0),
    )(inverse, me_col, joined_weight)
    known, sent = lax.optimization_barrier((known, sent))
    came = [sent[0]]
    for n in range(1, n_col):
        came.append(lax.ppermute(sent[n], "col", [(i, i ^ n) for i in range(n_col)]))
    known = gathered(known, "z")
    known_other = shifted(known, "core", 1)

    me = lax.axis_index(BOTH)
    row, col = me // 16, me % 16
    x, y, z, k = col // 2 % 4, col // 8 * 2 + row % 2, row // 2, col % 2
    at = jnp.arange(1024, dtype=jnp.int32)
    core = (k + at // 512) % 2
    first, second = at // 32 % 4, at // 8 % 4
    own_x = (x + jnp.where(core == 0, first, second)) % 4
    own_y = (y + jnp.where(core == 0, second, first)) % 4
    own_z = (z + at // 128 % 4) % 4
    owner = (own_z * 2 + own_y % 2) * 16 + (own_y // 2 * 4 + own_x) * 2 + core
    token = owner * 8 + at % 8

    expert_global = lax.axis_index("row") * local + jnp.arange(local, dtype=jnp.int32)
    weights = route_scores / jnp.sum(route_scores, axis=1, keepdims=True)
    share = jnp.sum(weights[:, :, None] * (expert_ids[:, :, None] == expert_global[None, None, :]), axis=1)
    share = jnp.take(share, token, axis=0)

    share = share.T
    known, known_other = (a.reshape(-1, a.shape[-1]) for a in (known, known_other))
    width = known.shape[1]

    def blocks(n, dtype):
        return jax.ShapeDtypeStruct((n, 8, width), dtype)

    vmem, hbm = pl.BlockSpec(memory_space=pltpu.VMEM), pl.BlockSpec(memory_space=pltpu.HBM)
    weights_in, other = pl.pallas_call(
        functools.partial(other_kernel, n_col),
        in_specs=[pl.BlockSpec(memory_space=pltpu.SMEM)] + [hbm] * (n_col + 1) + [vmem, vmem],
        out_specs=[vmem, vmem],
        out_shape=[jax.ShapeDtypeStruct((local, mine, width), jnp.bfloat16), blocks(64, jnp.bfloat16)],
        scratch_shapes=[
            pltpu.VMEM((n_col, mine, 384), jnp.bfloat16),
            pltpu.VMEM(known_other.shape, jnp.bfloat16),
            pltpu.SemaphoreType.DMA((n_col + 1,)),
        ],
        compiler_params=pltpu.CompilerParams(vmem_limit_bytes=32 << 20),
        name="other",
        cost_estimate=pl.CostEstimate(flops=4 << 30, bytes_accessed=16 << 20, transcendentals=1 << 18),
    )(me_col, *came, known_other, share[:, 512:], down_weight)
    came_over = shifted(other, "core", 1)
    act = hidden(weights_in, known, share[:, :512])
    outs = [blocks(16, f32)] + [blocks(16, jnp.bfloat16)] * 3
    total, *parts = own_call(act, down_weight, came_over, outs)
    weights_in, total = lax.optimization_barrier((weights_in, total))
    unit_major = jax.ShapeDtypeStruct((ff, local, width), jnp.bfloat16)
    gate_out, up_out = (
        a.transpose(1, 2, 0)
        for a in pl.pallas_call(
            emit_kernel,
            out_shape=[unit_major, unit_major],
            compiler_params=pltpu.CompilerParams(vmem_limit_bytes=20 << 20),
            name="emit",
            cost_estimate=pl.CostEstimate(flops=2 << 30, bytes_accessed=8 << 20, transcendentals=0),
        )(weights_in)
    )
    parts = [shifted(parts[by - 1], "first", by).astype(f32) for by in (1, 2, 3)]
    total = total + parts[0] + parts[1] + parts[2]
    total, gate_out, up_out = lax.optimization_barrier((total, gate_out, up_out))
    for axis, sent_as in (("second", jnp.bfloat16), ("z", f32)):
        total = total.reshape(4, -1, 8, width)
        parts = [shifted(total[by].astype(sent_as), axis, by).astype(f32) for by in (1, 2, 3)]
        total = total[0] + parts[0] + parts[1] + parts[2]
    total = total.reshape(8, width)
    return (gate_out, up_out, total.astype(jnp.bfloat16))


def solution(mesh):
    placed = (P("row", "col", None), P(), P("row", "col", None), P(("row", "col"), None), P(), P())
    return jax.shard_map(
        body,
        mesh=mesh,
        in_specs=placed,
        out_specs=(P("row", None, "col"), P("row", None, "col"), P(("row", "col"), None)),
        check_vma=False,
    )
```

```python
import functools

import jax
import jax.numpy as jnp
from jax import lax
from jax.experimental import pallas as pl
from jax.experimental.pallas import tpu as pltpu
from jax.sharding import PartitionSpec as P


BOTH = ("row", "col")


def place_of(i):
    row, col = divmod(i, 16)
    return col // 2 % 4, col // 8 * 2 + row % 2, row // 2, col % 2


def index_of(x, y, z, k):
    x, y, z = x % 4, y % 4, z % 4
    return (z * 2 + y % 2) * 16 + ((y // 2) * 4 + x) * 2 + k


def shifted(a, axis, by):
    pairs = []
    for i in range(128):
        x, y, z, k = place_of(i)
        if axis == "core":
            k = 1 - k
        elif axis == "z":
            z = z + by
        elif (axis == "first") == (k == 0):
            x = x + by
        else:
            y = y + by
        pairs.append((i, index_of(x, y, z, k)))
    return lax.ppermute(a.reshape(-1, 8, a.shape[-1]), BOTH, pairs)


def gathered(a, axis):
    far, near, back = (shifted(a, axis, -by) for by in (2, 1, 3))
    return jnp.concatenate([a.reshape(-1, 8, a.shape[-1]), near, far, back], axis=0)


def turn_kernel(tile_cols, inverse_ref, me_ref, x_ref, *refs):
    s_refs, (turned, staged, sems) = refs[:-3], refs[-3:]
    step = pl.program_id(0)
    local, depth, span = x_ref.shape
    half = tile_cols // 2
    tiles = s_refs[0].shape[0] // tile_cols
    lanes = 128
    same = lax.broadcasted_iota(jnp.int32, (lanes, lanes), 0) == lax.broadcasted_iota(jnp.int32, (lanes, lanes), 1)
    eye = jnp.where(same, 1.0, 0.0).astype(x_ref.dtype)

    gap = jnp.zeros((192 - depth, lanes), x_ref.dtype)
    for at in range(span // lanes):
        rows = pl.ds(pl.multiple_of(step * span + at * lanes, 8), lanes)
        part = slice(at * lanes, (at + 1) * lanes)
        stacked = jnp.concatenate([piece for e in range(local) for piece in (x_ref[e, :, part], gap)], axis=0)
        flipped = lax.dot_general(eye, stacked, (((1,), (1,)), ((), ())), preferred_element_type=jnp.float32)
        for lane in range(3):
            turned[lane, rows, :] = flipped[:, lane * lanes : (lane + 1) * lanes]

    @pl.when(step == pl.num_programs(0) - 1)
    def _():
        copies = []
        for n, s_ref in enumerate(s_refs):
            first = (me_ref[0] ^ n) * tiles
            starts = [inverse_ref[first + t] * tile_cols for t in range(tiles)]
            for lane in range(3):
                pieces = [
                    turned[lane, pl.ds(start + side, half, stride=2), :] for side in range(2) for start in starts
                ]
                whole = jnp.concatenate(pieces, axis=0).astype(staged.dtype)
                staged[n, :, lane * lanes : (lane + 1) * lanes] = whole
            copies.append(pltpu.make_async_copy(staged.at[n], s_ref, sems.at[n]))
            copies[-1].start()
        for copy in copies:
            copy.wait()


def activated(w, t, share):
    ff = w.shape[0] // 2
    pre = lax.dot_general(w, t, (((1,), (1,)), ((), ())), preferred_element_type=jnp.float32)
    gate, up = pre[:ff], pre[ff:]
    act = share * (up + 1.0) * gate * jax.nn.sigmoid(1.702 * gate)
    return act.astype(jnp.bfloat16).T


def hidden_kernel(w_ref, t_ref, share_ref, act_ref):
    for e in range(act_ref.shape[0]):
        act_ref[e] = activated(w_ref[e], t_ref[...], share_ref[e : e + 1, :])


def hidden(weights_in, tokens, share):
    local, mine, width = weights_in.shape
    rows, part = tokens.shape[0], 256
    return pl.pallas_call(
        hidden_kernel,
        grid=(rows // part,),
        in_specs=[
            pl.BlockSpec(weights_in.shape, lambda i: (0, 0, 0)),
            pl.BlockSpec((part, width), lambda i: (i, 0)),
            pl.BlockSpec((local, part), lambda i: (0, i)),
        ],
        out_specs=pl.BlockSpec((local, part, mine // 2), lambda i: (0, i, 0)),
        out_shape=jax.ShapeDtypeStruct((local, rows, mine // 2), jnp.bfloat16),
        compiler_params=pltpu.CompilerParams(vmem_limit_bytes=20 << 20),
        name="hidden",
        cost_estimate=pl.CostEstimate(flops=2 << 30, bytes_accessed=8 << 20, transcendentals=1 << 18),
    )(weights_in, tokens, share)


def projected(acts, downs):
    out = None
    for act, down in zip(acts, downs):
        term = jnp.dot(act, down, preferred_element_type=jnp.float32)
        out = term if out is None else out + term
    return out


def moved(block):
    return block % 16 * 4 + block // 16


def other_kernel(sources, me_ref, *refs):
    r_refs, (t_ref, share_ref, down_ref, w_ref, out_ref, r_in, t_in, sems) = refs[:sources], refs[sources:]
    local, _, width = down_ref.shape
    depth = width // sources
    for n, r_ref in enumerate(r_refs):
        slot = me_ref[0] ^ n
        pltpu.make_async_copy(r_ref, r_in.at[slot], sems.at[slot]).start()
    tokens_in = pltpu.make_async_copy(t_ref, t_in, sems.at[sources])
    tokens_in.start()
    for c in range(sources):
        pltpu.make_async_copy(r_refs[0], r_in.at[c], sems.at[c]).wait()
        for e in range(local):
            w_ref[e, :, c * depth : (c + 1) * depth] = r_in[c, :, e * 192 : e * 192 + depth]
    tokens_in.wait()
    acts = [activated(w_ref[e], t_in[...], share_ref[e : e + 1, :]) for e in range(local)]
    for at in range(0, width, 640):
        part = slice(at, min(at + 640, width))
        out = projected(acts, [down_ref[e, :, part] for e in range(local)])
        for block in range(out_ref.shape[0]):
            out_ref[moved(block), :, part] = out[block * 8 : (block + 1) * 8].astype(out_ref.dtype)


def emit_kernel(w_ref, gate_ref, up_ref):
    ff = gate_ref.shape[0]
    for e in range(w_ref.shape[0]):
        gate_ref[:, e, :] = w_ref[e, :ff, :]
        up_ref[:, e, :] = w_ref[e, ff:, :]


def own_kernel(act_ref, down_ref, came_ref, *out_refs):
    local, _, width = down_ref.shape
    acts = [act_ref[e] for e in range(local)]
    for at in range(0, width, 640):
        part = slice(at, min(at + 640, width))
        out = projected(acts, [down_ref[e, :, part] for e in range(local)])
        for block in range(came_ref.shape[0]):
            to = moved(block)
            both = out[block * 8 : (block + 1) * 8] + came_ref[to, :, part].astype(jnp.float32)
            ref = out_refs[to // 16]
            ref[to % 16, :, part] = both.astype(ref.dtype)


def own_call(act, down_weight, came, outs):
    vmem = pl.BlockSpec(memory_space=pltpu.VMEM)
    return pl.pallas_call(
        own_kernel,
        in_specs=[vmem] * 3,
        out_specs=[vmem] * len(outs),
        out_shape=outs,
        compiler_params=pltpu.CompilerParams(vmem_limit_bytes=20 << 20),
        name="down_own",
        cost_estimate=pl.CostEstimate(flops=1 << 30, bytes_accessed=8 << 20, transcendentals=0),
    )(act, down_weight, came)


def body(joined_weight, tile_perm, down_weight, tokens, expert_ids, route_scores):
    n_col = lax.axis_size("col")
    local, depth, width = joined_weight.shape
    tiles = tile_perm.shape[0]
    tile_cols = width // tiles
    mine = width // n_col
    ff = mine // 2
    span = 1152
    f32 = jnp.float32

    places = jnp.arange(tiles, dtype=jnp.int32)
    inverse = jnp.sum(places[:, None] * (tile_perm[:, None] == places[None, :]), axis=0)
    known = gathered(tokens, "second")
    known, inverse = lax.optimization_barrier((known, inverse))
    known = gathered(known, "first")
    me_col = lax.axis_index("col")[None]
    sent = pl.pallas_call(
        functools.partial(turn_kernel, tile_cols),
        grid_spec=pltpu.PrefetchScalarGridSpec(
            num_scalar_prefetch=2,
            grid=(width // span,),
            in_specs=[pl.BlockSpec((local, depth, span), lambda i, inv, me: (0, 0, i))],
            out_specs=[pl.BlockSpec(memory_space=pltpu.HBM)] * n_col,
            scratch_shapes=[
                pltpu.VMEM((3, width, 128), f32),
                pltpu.VMEM((n_col, mine, 384), jnp.bfloat16),
                pltpu.SemaphoreType.DMA((n_col,)),
            ],
        ),
        out_shape=[jax.ShapeDtypeStruct((mine, 384), jnp.bfloat16)] * n_col,
        compiler_params=pltpu.CompilerParams(vmem_limit_bytes=24 << 20),
        name="turn",
        cost_estimate=pl.CostEstimate(flops=4 << 30, bytes_accessed=16 << 20, transcendentals=0),
    )(inverse, me_col, joined_weight)
    known, sent = lax.optimization_barrier((known, sent))
    came = [sent[0]]
    for n in range(1, n_col):
        came.append(lax.ppermute(sent[n], "col", [(i, i ^ n) for i in range(n_col)]))
    known = gathered(known, "z")
    known_other = shifted(known, "core", 1)

    me = lax.axis_index(BOTH)
    row, col = me // 16, me % 16
    x, y, z, k = col // 2 % 4, col // 8 * 2 + row % 2, row // 2, col % 2
    at = jnp.arange(1024, dtype=jnp.int32)
    core = (k + at // 512) % 2
    first, second = at // 32 % 4, at // 8 % 4
    own_x = (x + jnp.where(core == 0, first, second)) % 4
    own_y = (y + jnp.where(core == 0, second, first)) % 4
    own_z = (z + at // 128 % 4) % 4
    owner = (own_z * 2 + own_y % 2) * 16 + (own_y // 2 * 4 + own_x) * 2 + core
    token = owner * 8 + at % 8

    expert_global = lax.axis_index("row") * local + jnp.arange(local, dtype=jnp.int32)
    weights = route_scores / jnp.sum(route_scores, axis=1, keepdims=True)
    share = jnp.sum(weights[:, :, None] * (expert_ids[:, :, None] == expert_global[None, None, :]), axis=1)
    share = jnp.take(share, token, axis=0)

    share = share.T
    known, known_other = (a.reshape(-1, a.shape[-1]) for a in (known, known_other))
    width = known.shape[1]

    def blocks(n, dtype):
        return jax.ShapeDtypeStruct((n, 8, width), dtype)

    vmem, hbm = pl.BlockSpec(memory_space=pltpu.VMEM), pl.BlockSpec(memory_space=pltpu.HBM)
    weights_in, other = pl.pallas_call(
        functools.partial(other_kernel, n_col),
        in_specs=[pl.BlockSpec(memory_space=pltpu.SMEM)] + [hbm] * (n_col + 1) + [vmem, vmem],
        out_specs=[vmem, vmem],
        out_shape=[jax.ShapeDtypeStruct((local, mine, width), jnp.bfloat16), blocks(64, jnp.bfloat16)],
        scratch_shapes=[
            pltpu.VMEM((n_col, mine, 384), jnp.bfloat16),
            pltpu.VMEM(known_other.shape, jnp.bfloat16),
            pltpu.SemaphoreType.DMA((n_col + 1,)),
        ],
        compiler_params=pltpu.CompilerParams(vmem_limit_bytes=32 << 20),
        name="other",
        cost_estimate=pl.CostEstimate(flops=4 << 30, bytes_accessed=16 << 20, transcendentals=1 << 18),
    )(me_col, *came, known_other, share[:, 512:], down_weight)
    came_over = shifted(other, "core", 1)
    act = hidden(weights_in, known, share[:, :512])
    outs = [blocks(16, f32)] + [blocks(16, jnp.bfloat16)] * 3
    total, *parts = own_call(act, down_weight, came_over, outs)
    weights_in, total = lax.optimization_barrier((weights_in, total))
    unit_major = jax.ShapeDtypeStruct((ff, local, width), jnp.bfloat16)
    gate_out, up_out = (
        a.transpose(1, 2, 0)
        for a in pl.pallas_call(
            emit_kernel,
            out_shape=[unit_major, unit_major],
            compiler_params=pltpu.CompilerParams(vmem_limit_bytes=20 << 20),
            name="emit",
            cost_estimate=pl.CostEstimate(flops=2 << 30, bytes_accessed=8 << 20, transcendentals=0),
        )(weights_in)
    )
    parts = [shifted(parts[by - 1], "first", by).astype(f32) for by in (2, 1, 3)]
    total = total + parts[0] + parts[1] + parts[2]
    total, gate_out, up_out = lax.optimization_barrier((total, gate_out, up_out))
    for axis, sent_as in (("second", jnp.bfloat16), ("z", f32)):
        total = total.reshape(4, -1, 8, width)
        parts = [shifted(total[by].astype(sent_as), axis, by).astype(f32) for by in (2, 1, 3)]
        total = total[0] + parts[0] + parts[1] + parts[2]
    total = total.reshape(8, width)
    return (gate_out, up_out, total.astype(jnp.bfloat16))


def solution(mesh):
    placed = (P("row", "col", None), P(), P("row", "col", None), P(("row", "col"), None), P(), P())
    return jax.shard_map(
        body,
        mesh=mesh,
        in_specs=placed,
        out_specs=(P("row", None, "col"), P("row", None, "col"), P(("row", "col"), None)),
        check_vma=False,
    )
```
